32 devices in a mesh: ens: 4 (over y, x), lon: 8 (over z, core).
Axes of the slice: x: 2, y: 2, z: 4, core: 2. Of those that a mesh axis runs over, the one named last changes fastest.
Arguments:
- control: float32 [8, 1024, 512], P('ens', None, 'lon'), may hold values from -6 to 6
- residual: float32 [8, 1024, 512], P('ens', None, 'lon'), may hold values from -6 to 6
- direction: float32 [8, 1024, 512], P('ens', None, 'lon'), may hold values from -6 to 6
- ens_perturb: bfloat16 [8, 3, 1024, 512], P('ens', None, None, 'lon'), may hold values from -1.5 to 1.5
- localize: float32 [1024, 1024], replicated, may hold values from -0.5 to 1.5
- obs_cell: int32 [32768], P('lon'), may hold values from 0 to 65535
- obs_slot: int32 [32768], P('lon'), may hold values from 0 to 3
- obs_weight: float32 [32768], P('lon'), may hold values from 0.5 to 4
Outputs:
- control_new: float32 [8, 1024, 512], P('ens', None, 'lon')
- residual_new: float32 [8, 1024, 512], P('ens', None, 'lon')
- direction_new: float32 [8, 1024, 512], P('ens', None, 'lon')
The draws below stay inside these ranges and needn't reach their ends.
Inputs may be any that keep to these rules, and one draw needn't show every extreme that they name: `obs_cell`: row-major cell within the entry's own longitude tile: row times 64 plus column. `obs_slot`: slot n < 3 observes the height after model step n + 1; slot 3 marks a padding entry that observes nothing.
All inputs are finite; a program needn't handle non-finite values.
Results may differ from the reference program's by a relative error of at most 0.0003.
Values sent between devices are 32-bit elements; how exact they have to be, the bound alone decides.
A program may use at most 64 MiB of HBM per device.

```python
import math
import jax
import jax.numpy as jnp
from jax import lax

LAT = 1024
CLON = 64
STEPS = 3
NOBS_DEV = 4096
MEMBERS = 8
LON = 512
NOBS = 32768


def draw_localize(key, part):
    row_ids = jnp.arange(LAT).astype(jnp.float32)
    distance = jnp.abs(row_ids[:, None] - row_ids[None, :])
    envelope = jnp.exp(-distance * 8.0 / LAT)
    jitter = 0.15 * jax.random.normal(key, (LAT, LAT), jnp.float32)
    jitter = jnp.clip(jitter, -0.5, 0.5)
    return jnp.eye(LAT, dtype=jnp.float32) + envelope * jitter


def place_ends(result, key, least, top_value):
    spot = [jax.random.randint(jax.random.fold_in(key, axis), (), 0, length) for axis, length in enumerate(result.shape)]
    main_axis = result.shape.index(max(result.shape))
    neighbour = spot[:main_axis] + [(spot[main_axis] + 1) % result.shape[main_axis]] + spot[main_axis + 1:]
    return result.at[tuple(spot)].set(least).at[tuple(neighbour)].set(top_value)


def levels(own_key, shape, split, least, largest):
    gain, own = 1.0, jax.random.fold_in(own_key, 6)
    for axis_at, blocks in split:
        draws = jnp.exp(jax.random.uniform(jax.random.fold_in(own, axis_at), (blocks,), jnp.float32, least / len(split), largest / len(split)))
        gain = gain * jnp.repeat(draws, shape[axis_at] // blocks).reshape([-1 if axis == axis_at else 1 for axis in range(len(shape))])
    return gain


def normal_values(own_key, dims, deviation, bound, split=(), held_as=jnp.bfloat16):
    gain = levels(own_key, dims, split, -0.22, 0.18) if split else 1.0
    result = jax.random.normal(own_key, dims, jnp.float32) * deviation * gain
    return jnp.minimum(jnp.maximum(result, -bound), bound).astype(held_as)


def setup_inputs(seed: int = 0) -> dict:
    keys = jax.random.split(jax.random.key(seed), 9)
    control = normal_values(keys[0], (MEMBERS, LAT, LON), 1.0, 6.0, ((0, 4), (2, 8)), jnp.float32)
    residual = normal_values(keys[1], (MEMBERS, LAT, LON), 1.0, 6.0, ((0, 4), (2, 8)), jnp.float32)
    direction = normal_values(keys[2], (MEMBERS, LAT, LON), 1.0, 6.0, ((0, 4), (2, 8)), jnp.float32)
    ens_perturb = normal_values(keys[3], (MEMBERS, 3, LAT, LON), 0.25, 1.5, ((0, 4), (3, 8)))
    localize = draw_localize(jax.random.fold_in(keys[8], 71), 0)
    obs_cell = place_ends(jax.random.randint(keys[5], (NOBS,), 0, LAT * CLON), jax.random.fold_in(keys[5], 1), 0, (LAT * CLON) - 1).astype(jnp.int32)
    obs_slot = place_ends(jax.random.randint(keys[6], (NOBS,), 0, STEPS + 1), jax.random.fold_in(keys[6], 1), 0, STEPS).astype(jnp.int32)
    obs_weight = jnp.clip(jnp.exp(math.log(4.0) - 2.0794415 * jax.random.uniform(keys[7], (NOBS,), jnp.float32) ** levels(keys[7], (NOBS,), ((0, 8),), -0.2, 0.2)), 0.5, 4.0)
    return {"control": control, "residual": residual, "direction": direction, "ens_perturb": ens_perturb, "localize": localize, "obs_cell": obs_cell, "obs_slot": obs_slot, "obs_weight": obs_weight}


wave_speed = 0.35
rotation = 0.2

def grid_factors(row_ids, lat_total):
    latitude = (-1.0 / 3.0 + 2.0 / 3.0 * (row_ids + 0.5) / lat_total) * jnp.pi
    return (1.0 / jnp.cos(latitude), jnp.sin(latitude))

def linear_step(fields, orient, metric, coriolis):
    height, zonal, meridional = (fields[0], fields[1], fields[2])

    def lon_diff(values):
        return 0.5 * metric[:, None] * (jnp.roll(values, -1, axis=1) - jnp.roll(values, 1, axis=1))

    def lat_diff(values):
        widened = jnp.pad(values, ((1, 1), (0, 0)))
        return 0.5 * (widened[2:] - widened[:-2])
    speed = orient * wave_speed
    turning = orient * rotation * coriolis[:, None]
    return jnp.stack([height - speed * (lon_diff(zonal) + lat_diff(meridional)), zonal - speed * lon_diff(height) + turning * meridional, meridional - speed * lat_diff(height) - turning * zonal])

def reference(control, residual, direction, ens_perturb, localize, obs_cell, obs_slot, obs_weight):
    hi = lax.Precision.HIGHEST
    row_ids = jnp.arange(LAT).astype(jnp.float32)
    metric, coriolis = grid_factors(row_ids, LAT)
    tile_index = (jnp.arange(obs_cell.shape[0]) // NOBS_DEV).astype(jnp.int32)
    cell_index = (obs_cell // CLON * LON + tile_index * CLON + obs_cell % CLON).astype(jnp.int32)

    def member_inc(accum, member_pair):
        member_pert, member_vec = member_pair
        localized = jnp.dot(localize, member_vec, precision=hi)
        return (accum + member_pert.astype(jnp.float32) * localized[None], None)
    increment, _ = lax.scan(member_inc, jnp.zeros((3, LAT, LON), jnp.float32), (ens_perturb, direction))
    tl_state = increment
    observed = jnp.zeros(obs_cell.shape, jnp.float32)
    for moment in range(STEPS):
        tl_state = linear_step(tl_state, 1.0, metric, coriolis)
        sampled = tl_state[0].reshape(-1)[cell_index]
        observed = jnp.where(obs_slot == moment, sampled, observed)
    weighted = obs_weight * observed
    adjoint = jnp.zeros((3, LAT, LON), jnp.float32)
    for moment in reversed(range(STEPS)):
        forcing = jnp.zeros((LAT * LON,), jnp.float32).at[cell_index].add(jnp.where(obs_slot == moment, weighted, 0.0))
        adjoint = adjoint.at[0].add(forcing.reshape(LAT, LON))
        adjoint = linear_step(adjoint, -1.0, metric, coriolis)

    def member_grad(carried, member_pert):
        projected = lax.optimization_barrier(jnp.sum(member_pert.astype(jnp.float32) * adjoint, axis=0))
        return (carried, jnp.dot(localize.T, projected, precision=hi))
    _, pulled_back = lax.scan(member_grad, jnp.float32(0.0), ens_perturb)
    image_vec = direction + pulled_back
    norm_old = jnp.sum(residual * residual)
    step_size = norm_old / jnp.sum(direction * image_vec)
    control_new = control + step_size * direction
    residual_new = residual - step_size * image_vec
    norm_new = jnp.sum(residual_new * residual_new)
    direction_new = residual_new + norm_new / norm_old * direction
    return (control_new, residual_new, direction_new)
```

```python
import functools

import numpy as np
import jax
import jax.numpy as jnp
from jax import lax
from jax.experimental import pallas as pl
from jax.experimental.pallas import tpu as pltpu
from jax.sharding import PartitionSpec as P

STEPS = 3
HALO = 8
CHUNK = 512
MESH = pl.DeviceIdType.MESH
NT = (((1,), (1,)), ((), ()))
NN = (((1,), (0,)), ((), ()))


def split_bf16(values):
    high = values.astype(jnp.bfloat16)
    low = (values - high.astype(jnp.float32)).astype(jnp.bfloat16)
    return high, low


def dot(left, right, dims):
    return lax.dot_general(left, right, dims, preferred_element_type=jnp.float32)


def grid_constants(lat):
    phi = np.pi * (-1.0 / 3.0 + 2.0 / 3.0 * (np.arange(lat) + 0.5) / lat)
    half = 0.5 * 0.35
    up = np.full(lat, half)
    up[-1] = 0.0
    down = np.full(lat, half)
    down[0] = 0.0
    rows = np.stack([half / np.cos(phi), 0.2 * np.sin(phi), up, down])
    return np.ascontiguousarray(np.broadcast_to(rows[:, None], (4, 8, lat))).astype(np.float32)


def linear_step(source, target, sign, consts, forcing=None):
    rows, lat = source.shape[1], source.shape[2]
    lon_c, cor_c, up_c, down_c = (sign * consts[k] for k in range(4))
    for start in range(0, rows, 8):
        here = pl.ds(start, 8)

        def east(comp, block):
            if start + 8 == rows:
                return pltpu.roll(block, 7, 0)
            return source[comp, pl.ds(start + 1, 8), :]

        def west(comp, block):
            if start == 0:
                return pltpu.roll(block, 1, 0)
            return source[comp, pl.ds(start - 1, 8), :]

        def lat_diff(block):
            return up_c * pltpu.roll(block, lat - 1, 1) - down_c * pltpu.roll(block, 1, 1)

        height, zonal, merid = (source[c, here, :] for c in range(3))
        height_lon = east(0, height) - west(0, height)
        zonal_lon = east(1, zonal) - west(1, zonal)
        target[0, here, :] = height - lon_c * zonal_lon - lat_diff(merid)
        target[1, here, :] = zonal - lon_c * height_lon + cor_c * merid
        target[2, here, :] = merid - lat_diff(height) - cor_c * zonal


def kernel(
    ens, lon, direction, residual, perturb, localize, cell, slot, weight, consts,
    image, scalars,
    high, low, split, stage, arrived, reduced, fields, other, heights, wsum, wmat,
    tiles, tile,
    rs_send, rs_recv, ag_send, ag_recv, halo_send, halo_recv, tile_send, tile_recv,
):
    me_e, me_l = lax.axis_index("ens"), lax.axis_index("lon")
    count = ens * lon
    me = me_e * lon + me_l
    members, cols, lat = direction.shape
    block = lat // ens
    stacked = members * cols

    barrier = pltpu.get_barrier_semaphore()

    def greet(offset, carry):
        peer = lax.rem(me + offset, count)
        pl.semaphore_signal(
            barrier, inc=1, device_id=(peer // lon, lax.rem(peer, lon)), device_id_type=MESH
        )
        return carry

    lax.fori_loop(1, count, greet, 0)

    d_high, d_low = split_bf16(direction[...].reshape(stacked, lat))
    split[pl.ds(0, stacked), :] = d_high
    split[pl.ds(stacked, stacked), :] = d_low

    def localized_block(index, dest):
        at = pl.ds(pl.multiple_of(index * block, block), block)
        l_high, l_low = split_bf16(localize[at, :])
        high[at, :] = l_high
        low[at, :] = l_low
        both = dot(split[...], l_high, NT)
        local = both[:stacked] + both[stacked:] + dot(split[pl.ds(0, stacked), :], l_low, NT)
        for c in range(3):
            total = None
            for m in range(members):
                term = perturb[m, c, :, at].astype(jnp.float32) * local[m * cols:(m + 1) * cols]
                total = term if total is None else total + term
            stage[dest, c] = total

    def peer_of(offset):
        return lax.rem(me_e + offset, ens)

    def first(offset, carry):
        localized_block(peer_of(offset), offset - 1)
        return carry

    def rs_copy(offset, c):
        return pltpu.make_async_remote_copy(
            src_ref=stage.at[offset - 1, c], dst_ref=arrived.at[offset - 1, c],
            send_sem=rs_send.at[offset - 1, c], recv_sem=rs_recv.at[offset - 1, c],
            device_id=(peer_of(offset), me_l), device_id_type=MESH,
        )

    localized_block(peer_of(1), 0)
    pl.semaphore_wait(barrier, count - 1)
    for c in range(3):
        rs_copy(1, c).start()
    for offset in range(2, ens):
        localized_block(peer_of(offset), offset - 1)
        for c in range(3):
            rs_copy(offset, c).start()
    localized_block(me_e, ens - 1)

    wsum[...] = jnp.zeros_like(wsum)
    slots_cols = STEPS * cols

    def weights(step, carry):
        at = pl.ds(pl.multiple_of(step * CHUNK, CHUNK), CHUNK)
        cells, slots, value = cell[:, at], slot[:, at], weight[:, at]
        row = cells // cols
        key = slots * cols + (cells - row * cols)
        v_high, v_low = split_bf16(value)
        v_high, v_low = v_high.astype(jnp.float32), v_low.astype(jnp.float32)
        ids = lax.broadcasted_iota(jnp.int32, (slots_cols, CHUNK), 0)
        hit = ids == key
        left = jnp.concatenate(
            [jnp.where(hit, v_high, 0.0), jnp.where(hit, v_low, 0.0)], axis=0
        ).astype(jnp.bfloat16)
        lat_ids = lax.broadcasted_iota(jnp.int32, (lat, CHUNK), 0)
        right = jnp.where(lat_ids == row, 1.0, 0.0).astype(jnp.bfloat16)
        wsum[...] += dot(left, right, NT)
        return carry

    lax.fori_loop(0, cell.shape[1] // CHUNK, weights, 0)
    for s in range(STEPS):
        wmat[s, pl.ds(HALO, cols), :] = (
            wsum[pl.ds(s * cols, cols), :] + wsum[pl.ds(slots_cols + s * cols, cols), :]
        )

    left_dev = (me_e, lax.rem(me_l + lon - 1, lon))
    right_dev = (me_e, lax.rem(me_l + 1, lon))

    def halo_copies(ref, which):
        west = pltpu.make_async_remote_copy(
            src_ref=ref.at[:, pl.ds(HALO, HALO), :], dst_ref=ref.at[:, pl.ds(HALO + cols, HALO), :],
            send_sem=halo_send.at[which, 0], recv_sem=halo_recv.at[which, 0],
            device_id=left_dev, device_id_type=MESH,
        )
        east = pltpu.make_async_remote_copy(
            src_ref=ref.at[:, pl.ds(cols, HALO), :], dst_ref=ref.at[:, pl.ds(0, HALO), :],
            send_sem=halo_send.at[which, 1], recv_sem=halo_recv.at[which, 1],
            device_id=right_dev, device_id_type=MESH,
        )
        return west, east

    w_copies = halo_copies(wmat, 0)
    for copy in w_copies:
        copy.start()

    mine = pl.ds(pl.multiple_of(me_e * block, block), block)

    def ag_copy(offset, c):
        return pltpu.make_async_remote_copy(
            src_ref=reduced.at[c], dst_ref=fields.at[c, pl.ds(HALO, cols), mine],
            send_sem=ag_send.at[offset - 1, c], recv_sem=ag_recv.at[offset - 1, c],
            device_id=(peer_of(offset), me_l), device_id_type=MESH,
        )

    for c in range(3):
        total = stage[ens - 1, c]
        for offset in range(1, ens):
            rs_copy(offset, c).wait_recv()
            total = total + arrived[offset - 1, c]
        reduced[c] = total
        fields[c, pl.ds(HALO, cols), mine] = total
        for offset in range(1, ens):
            ag_copy(offset, c).start()
    for c in range(3):
        for offset in range(1, ens):
            ag_copy(offset, c).wait_recv()

    f_copies = halo_copies(fields, 1)
    for copy in f_copies:
        copy.start()
    for copy in f_copies:
        copy.wait()

    def forward(source, target, n):
        linear_step(source, target, 1.0, consts)
        heights[n] = target[0]

    forward(fields, other, 0)
    forward(other, fields, 1)
    forward(fields, other, 2)
    for copy in w_copies:
        copy.wait()
    fields[0] = wmat[2] * heights[2]
    fields[1] = jnp.zeros_like(fields[1])
    fields[2] = jnp.zeros_like(fields[2])
    linear_step(fields, other, -1.0, consts)
    other[0] += wmat[1] * heights[1]
    linear_step(other, fields, -1.0, consts)
    fields[0] += wmat[0] * heights[0]
    linear_step(fields, other, -1.0, consts)

    for m in range(members):
        total = None
        for c in range(3):
            term = perturb[m, c].astype(jnp.float32) * other[c, pl.ds(HALO, cols), :]
            total = term if total is None else total + term
        p_high, p_low = split_bf16(total)
        split[pl.ds(m * cols, cols), :] = p_high
        split[pl.ds(stacked + m * cols, cols), :] = p_low

    def pulled(index, sums):
        at = pl.ds(pl.multiple_of(index * block, block), block)
        both = dot(split[...], high[:, at], NN)
        back = both[:stacked] + both[stacked:] + dot(split[pl.ds(0, stacked), :], low[:, at], NN)
        out = []
        d = direction[:, :, at].reshape(stacked, block)
        r = residual[:, :, at].reshape(stacked, block)
        img = d + back
        image[:, :, at] = img.reshape(members, cols, block)
        for total, term in zip(sums, (r * r, d * img, r * img, img * img)):
            term = term.reshape(stacked // 8, 8, block).sum(axis=0)
            for k in range(block // 128):
                total = total + term[:, k * 128:(k + 1) * 128]
            out.append(total)
        return tuple(out)

    sums = lax.fori_loop(0, ens, pulled, tuple(jnp.zeros((8, 128), jnp.float32) for _ in range(4)))
    rows = [jnp.sum(s, axis=0, keepdims=True) for s in sums]
    tile[...] = jnp.concatenate(rows + [jnp.zeros((4, 128), jnp.float32)], axis=0)

    def tell(offset, carry):
        peer = lax.rem(me + offset, count)
        pltpu.make_async_remote_copy(
            src_ref=tile, dst_ref=tiles.at[offset - 1],
            send_sem=tile_send, recv_sem=tile_recv,
            device_id=(peer // lon, lax.rem(peer, lon)), device_id_type=MESH,
        ).start()
        return carry

    lax.fori_loop(1, count, tell, 0)
    for c in range(3):
        for offset in range(1, ens):
            rs_copy(offset, c).wait_send()
            ag_copy(offset, c).wait_send()
    everything = pltpu.make_async_remote_copy(
        src_ref=tiles, dst_ref=tiles, send_sem=tile_send, recv_sem=tile_recv,
        device_id=right_dev, device_id_type=MESH,
    )
    everything.wait_send()
    everything.wait_recv()
    total = jnp.sum(tiles[...], axis=0) + tile[...]
    scalars[...] = jnp.broadcast_to(jnp.sum(total, axis=1, keepdims=True), (8, 128))


def body(ens, lon, control, residual, direction, ens_perturb, localize, obs_cell, obs_slot, obs_weight):
    flip = functools.partial(jnp.swapaxes, axis1=-1, axis2=-2)
    control, residual, direction, ens_perturb = map(flip, (control, residual, direction, ens_perturb))
    members, cols, lat = direction.shape
    nobs = obs_cell.shape[0]
    block = lat // ens
    count = ens * lon
    wide = cols + 2 * HALO
    f32, bf16 = jnp.float32, jnp.bfloat16
    vmem = pl.BlockSpec(memory_space=pltpu.VMEM)
    dma = pltpu.SemaphoreType.DMA
    image, scalars = pl.pallas_call(
        functools.partial(kernel, ens, lon),
        out_shape=(
            jax.ShapeDtypeStruct((members, cols, lat), f32),
            jax.ShapeDtypeStruct((8, 128), f32),
        ),
        in_specs=[vmem] * 8,
        out_specs=(vmem, vmem),
        scratch_shapes=[
            pltpu.VMEM((lat, lat), bf16),
            pltpu.VMEM((lat, lat), bf16),
            pltpu.VMEM((2 * members * cols, lat), bf16),
            pltpu.VMEM((ens, 3, cols, block), f32),
            pltpu.VMEM((ens - 1, 3, cols, block), f32),
            pltpu.VMEM((3, cols, block), f32),
            pltpu.VMEM((3, wide, lat), f32),
            pltpu.VMEM((3, wide, lat), f32),
            pltpu.VMEM((STEPS, wide, lat), f32),
            pltpu.VMEM((2 * STEPS * cols, lat), f32),
            pltpu.VMEM((STEPS, wide, lat), f32),
            pltpu.VMEM((count - 1, 8, 128), f32),
            pltpu.VMEM((8, 128), f32),
            dma((ens - 1, 3)), dma((ens - 1, 3)),
            dma((ens - 1, 3)), dma((ens - 1, 3)),
            dma((2, 2)), dma((2, 2)),
            dma, dma,
        ],
        compiler_params=pltpu.CompilerParams(collective_id=0, has_side_effects=True),
    )(
        direction, residual, ens_perturb, localize,
        obs_cell.reshape(1, nobs), obs_slot.reshape(1, nobs), obs_weight.reshape(1, nobs),
        jnp.asarray(grid_constants(lat)),
    )
    norm_old, curvature, cross_term, square = (scalars[k, 0] for k in range(4))
    step_size = norm_old / curvature
    control_new = control + step_size * direction
    residual_new = residual - step_size * image
    norm_new = norm_old - 2.0 * step_size * cross_term + step_size * step_size * square
    direction_new = residual_new + norm_new / norm_old * direction
    return tuple(map(flip, (control_new, residual_new, direction_new)))


def solution(mesh):
    fields = P("ens", None, "lon")
    in_specs = (fields, fields, fields, P("ens", None, None, "lon"), P(), P("lon"), P("lon"), P("lon"))
    ens, lon = mesh.shape["ens"], mesh.shape["lon"]
    return jax.shard_map(
        functools.partial(body, ens, lon), mesh=mesh, in_specs=in_specs,
        out_specs=(fields, fields, fields), check_vma=False,
    )
```

```python
import functools
import itertools

import numpy as np
import jax
import jax.numpy as jnp
from jax import lax
from jax.experimental import pallas as pl
from jax.experimental.pallas import tpu as pltpu
from jax.sharding import PartitionSpec as P

STEPS = 3
HALO = 8
CHUNK = 512
MESH = pl.DeviceIdType.MESH
NT = (((1,), (1,)), ((), ()))
NN = (((1,), (0,)), ((), ()))


def split_bf16(values):
    high = values.astype(jnp.bfloat16)
    low = (values - high.astype(jnp.float32)).astype(jnp.bfloat16)
    return high, low


def dot(left, right, dims):
    return lax.dot_general(left, right, dims, preferred_element_type=jnp.float32)


def grid_constants(lat):
    phi = np.pi * (-1.0 / 3.0 + 2.0 / 3.0 * (np.arange(lat) + 0.5) / lat)
    half = 0.5 * 0.35
    up = np.full(lat, half)
    up[-1] = 0.0
    down = np.full(lat, half)
    down[0] = 0.0
    rows = np.stack([half / np.cos(phi), 0.2 * np.sin(phi), up, down])
    return np.ascontiguousarray(np.broadcast_to(rows[:, None], (4, 8, lat))).astype(np.float32)


def linear_step(source, target, sign, consts, forcing=None):
    rows, lat = source.shape[1], source.shape[2]
    lon_c, cor_c, up_c, down_c = (sign * consts[k] for k in range(4))
    for start in range(0, rows, 8):
        here = pl.ds(start, 8)

        def east(comp, block):
            if start + 8 == rows:
                return pltpu.roll(block, 7, 0)
            return source[comp, pl.ds(start + 1, 8), :]

        def west(comp, block):
            if start == 0:
                return pltpu.roll(block, 1, 0)
            return source[comp, pl.ds(start - 1, 8), :]

        def lat_diff(block):
            return up_c * pltpu.roll(block, lat - 1, 1) - down_c * pltpu.roll(block, 1, 1)

        height, zonal, merid = (source[c, here, :] for c in range(3))
        height_lon = east(0, height) - west(0, height)
        zonal_lon = east(1, zonal) - west(1, zonal)
        target[0, here, :] = height - lon_c * zonal_lon - lat_diff(merid)
        target[1, here, :] = zonal - lon_c * height_lon + cor_c * merid
        target[2, here, :] = merid - lat_diff(height) - cor_c * zonal


def factors(ens):
    first = 2 if ens % 2 == 0 else 1
    return first, ens // first


def copy_count(ens):
    na, nb = factors(ens)
    cross = (na - 1) * (nb - 1)
    return 3 * (4 * cross + 3 * (na - 1 + nb - 1)) + 8


def kernel(
    ens, lon, direction, residual_hbm, perturb_hbm, localize_hbm, cell, slot, weight, consts,
    image, step_row, ratio_row,
    localize, residual, perturb, high, low, split, stage, relay0, relay1, arr_a, arr_b,
    reduced, fields, other, heights, wsum, wmat, tiles, tile,
    load_sem, send_sem, recv_sem, tile_send, tile_recv,
):
    na, nb = factors(ens)
    me_e, me_l = lax.axis_index("ens"), lax.axis_index("lon")
    me_a, me_b = me_e // nb, lax.rem(me_e, nb)
    count = ens * lon
    me = me_e * lon + me_l
    members, cols, lat = direction.shape
    block = lat // ens
    half = cols // 2
    stacked = members * cols
    halves = (pl.ds(0, half), pl.ds(half, half))
    inner = (pl.ds(HALO, half), pl.ds(HALO + half, half))

    def ens_of(i, j):
        return lax.rem(me_a + i, na) * nb + lax.rem(me_b + j, nb)

    def lanes_of(index):
        return pl.ds(pl.multiple_of(index * block, block), block)

    order = [(i, j) for i in range(1, na) for j in range(1, nb)]
    order += [(0, j) for j in range(1, nb)] + [(i, 0) for i in range(1, na)] + [(0, 0)]

    loads = {}
    for k, (i, j) in enumerate(order):
        at = lanes_of(ens_of(i, j))
        loads[i, j] = pltpu.make_async_copy(localize_hbm.at[at, :], localize.at[at, :], load_sem.at[k])
    load_p = pltpu.make_async_copy(perturb_hbm, perturb, load_sem.at[ens])
    load_r = pltpu.make_async_copy(residual_hbm, residual, load_sem.at[ens + 1])
    loads[order[0]].start()
    load_p.start()
    for key in order[1:]:
        loads[key].start()
    load_r.start()

    barrier = pltpu.get_barrier_semaphore()

    def greet(offset, carry):
        peer = lax.rem(me + offset, count)
        pl.semaphore_signal(
            barrier, inc=1, device_id=(peer // lon, lax.rem(peer, lon)), device_id_type=MESH
        )
        return carry

    lax.fori_loop(1, count, greet, 0)

    ids = itertools.count()

    def remote(src, dst, device):
        k = next(ids)
        return pltpu.make_async_remote_copy(
            src_ref=src, dst_ref=dst, send_sem=send_sem.at[k], recv_sem=recv_sem.at[k],
            device_id=device, device_id_type=MESH,
        )

    d_high, d_low = split_bf16(direction[...].reshape(stacked, lat))
    split[pl.ds(0, stacked), :] = d_high
    split[pl.ds(stacked, stacked), :] = d_low

    def localized_block(i, j):
        index = ens_of(i, j)
        at = lanes_of(index)
        loads[i, j].wait()
        l_high, l_low = split_bf16(localize[at, :])
        high[at, :] = l_high
        low[at, :] = l_low
        both = dot(split[...], l_high, NT)
        local = both[:stacked] + both[stacked:] + dot(split[pl.ds(0, stacked), :], l_low, NT)
        if (i, j) == order[0]:
            load_p.wait()
        for c in range(3):
            total = None
            for m in range(members):
                term = perturb[m, c, :, at].astype(jnp.float32) * local[m * cols:(m + 1) * cols]
                total = term if total is None else total + term
            stage[i * nb + j, c] = total

    def a_peer(i):
        return (ens_of(i, 0), me_l)

    def b_peer(j):
        return (ens_of(0, j), me_l)

    def part(i, j, c, h):
        return stage.at[i * nb + j, c, halves[h]]

    sum0, sum1, direct, relayed0, relayed1 = {}, {}, {}, {}, {}
    for c in range(3):
        for i in range(1, na):
            for j in range(1, nb):
                sum0[i, j, c] = remote(part(i, j, c, 0), relay0.at[j - 1, i - 1, c], b_peer(j))
                sum1[i, j, c] = remote(part(i, j, c, 1), relay1.at[i - 1, j - 1, c], a_peer(i))
        for j in range(1, nb):
            direct[0, j, c] = remote(part(0, j, c, 0), arr_b.at[j - 1, c, halves[0]], b_peer(j))
            relayed1[j, c] = remote(part(0, j, c, 1), arr_b.at[j - 1, c, halves[1]], b_peer(j))
        for i in range(1, na):
            direct[i, 0, c] = remote(part(i, 0, c, 1), arr_a.at[i - 1, c, halves[1]], a_peer(i))
            relayed0[i, c] = remote(part(i, 0, c, 0), arr_a.at[i - 1, c, halves[0]], a_peer(i))

    for k, (i, j) in enumerate(order):
        localized_block(i, j)
        if k == 0:
            pl.semaphore_wait(barrier, count - 1)
        for c in range(3):
            if i and j:
                sum0[i, j, c].start()
                sum1[i, j, c].start()
            elif i or j:
                direct[i, j, c].start()

    wsum[...] = jnp.zeros_like(wsum)
    slots_cols = STEPS * cols

    def weights(step, carry):
        at = pl.ds(pl.multiple_of(step * CHUNK, CHUNK), CHUNK)
        cells, slots, value = cell[:, at], slot[:, at], weight[:, at]
        row = cells // cols
        key = slots * cols + (cells - row * cols)
        v_high, v_low = split_bf16(value)
        v_high, v_low = v_high.astype(jnp.float32), v_low.astype(jnp.float32)
        ids = lax.broadcasted_iota(jnp.int32, (slots_cols, CHUNK), 0)
        hit = ids == key
        left = jnp.concatenate(
            [jnp.where(hit, v_high, 0.0), jnp.where(hit, v_low, 0.0)], axis=0
        ).astype(jnp.bfloat16)
        lat_ids = lax.broadcasted_iota(jnp.int32, (lat, CHUNK), 0)
        right = jnp.where(lat_ids == row, 1.0, 0.0).astype(jnp.bfloat16)
        wsum[...] += dot(left, right, NT)
        return carry

    chunks = cell.shape[1] // CHUNK
    early = chunks // 2
    lax.fori_loop(0, early, weights, 0)

    for c in range(3):
        for i in range(1, na):
            for j in range(1, nb):
                sum0[i, j, c].wait_recv()
                stage[i * nb, c, halves[0]] += relay0[j - 1, i - 1, c]
            relayed0[i, c].start()
        for j in range(1, nb):
            for i in range(1, na):
                sum1[i, j, c].wait_recv()
                stage[j, c, halves[1]] += relay1[i - 1, j - 1, c]
            relayed1[j, c].start()

    lax.fori_loop(early, chunks, weights, 0)
    for s in range(STEPS):
        wmat[s, pl.ds(HALO, cols), :] = (
            wsum[pl.ds(s * cols, cols), :] + wsum[pl.ds(slots_cols + s * cols, cols), :]
        )

    left_dev = (me_e, lax.rem(me_l + lon - 1, lon))
    right_dev = (me_e, lax.rem(me_l + 1, lon))

    def halo_copies(ref, which):
        return (
            remote(ref.at[which, pl.ds(HALO, HALO), :], ref.at[which, pl.ds(HALO + cols, HALO), :], left_dev),
            remote(ref.at[which, pl.ds(cols, HALO), :], ref.at[which, pl.ds(0, HALO), :], right_dev),
        )

    w_copies = (
        remote(wmat.at[:, pl.ds(HALO, HALO), :], wmat.at[:, pl.ds(HALO + cols, HALO), :], left_dev),
        remote(wmat.at[:, pl.ds(cols, HALO), :], wmat.at[:, pl.ds(0, HALO), :], right_dev),
    )
    for copy in w_copies:
        copy.start()

    mine = lanes_of(me_e)
    own_a, own_b, pass_a, pass_b = {}, {}, {}, {}
    for c in range(3):
        whole = fields.at[c, pl.ds(HALO, cols), mine]
        for i in range(1, na):
            own_a[i, c] = remote(reduced.at[c], whole, a_peer(i))
        for j in range(1, nb):
            own_b[j, c] = remote(reduced.at[c], whole, b_peer(j))
        for i in range(1, na):
            for j in range(1, nb):
                from_b = lanes_of(me_a * nb + lax.rem(me_b + nb - j, nb))
                from_a = lanes_of(lax.rem(me_a + na - i, na) * nb + me_b)
                spot0 = fields.at[c, inner[0], from_b]
                spot1 = fields.at[c, inner[1], from_a]
                pass_a[i, j, c] = remote(spot0, spot0, a_peer(i))
                pass_b[i, j, c] = remote(spot1, spot1, b_peer(j))

    for c in range(3):
        total = stage[0, c]
        for j in range(1, nb):
            direct[0, j, c].wait_recv()
            relayed1[j, c].wait_recv()
            total = total + arr_b[j - 1, c]
        for i in range(1, na):
            direct[i, 0, c].wait_recv()
            relayed0[i, c].wait_recv()
            total = total + arr_a[i - 1, c]
        reduced[c] = total
        fields[c, pl.ds(HALO, cols), mine] = total
        for copy in [own_a[i, c] for i in range(1, na)] + [own_b[j, c] for j in range(1, nb)]:
            copy.start()
    load_r.wait()
    for c in range(3):
        for j in range(1, nb):
            own_b[j, c].wait_recv()
            for i in range(1, na):
                pass_a[i, j, c].start()
        for i in range(1, na):
            own_a[i, c].wait_recv()
            for j in range(1, nb):
                pass_b[i, j, c].start()
    f_copies = []
    for c in range(3):
        for i in range(1, na):
            for j in range(1, nb):
                pass_a[i, j, c].wait_recv()
                pass_b[i, j, c].wait_recv()
        for copy in halo_copies(fields, c):
            copy.start()
            f_copies.append(copy)
    for group in (pass_a, pass_b):
        for copy in group.values():
            copy.wait_send()
    for copy in f_copies:
        copy.wait()

    def forward(source, target, n):
        linear_step(source, target, 1.0, consts)
        heights[n] = target[0]

    forward(fields, other, 0)
    forward(other, fields, 1)
    forward(fields, other, 2)
    for copy in w_copies:
        copy.wait()
    fields[0] = wmat[2] * heights[2]
    fields[1] = jnp.zeros_like(fields[1])
    fields[2] = jnp.zeros_like(fields[2])
    linear_step(fields, other, -1.0, consts)
    other[0] += wmat[1] * heights[1]
    linear_step(other, fields, -1.0, consts)
    fields[0] += wmat[0] * heights[0]
    linear_step(fields, other, -1.0, consts)

    for m in range(members):
        total = None
        for c in range(3):
            term = perturb[m, c].astype(jnp.float32) * other[c, pl.ds(HALO, cols), :]
            total = term if total is None else total + term
        p_high, p_low = split_bf16(total)
        split[pl.ds(m * cols, cols), :] = p_high
        split[pl.ds(stacked + m * cols, cols), :] = p_low

    def pulled(index, sums):
        at = lanes_of(index)
        both = dot(split[...], high[:, at], NN)
        back = both[:stacked] + both[stacked:] + dot(split[pl.ds(0, stacked), :], low[:, at], NN)
        out = []
        d = direction[:, :, at].reshape(stacked, block)
        r = residual[:, :, at].reshape(stacked, block)
        img = d + back
        image[:, :, at] = img.reshape(members, cols, block)
        for total, term in zip(sums, (r * r, d * img, r * img, img * img)):
            term = term.reshape(stacked // 8, 8, block).sum(axis=0)
            for k in range(block // 128):
                total = total + term[:, k * 128:(k + 1) * 128]
            out.append(total)
        return tuple(out)

    sums = lax.fori_loop(0, ens, pulled, tuple(jnp.zeros((8, 128), jnp.float32) for _ in range(4)))
    rows = [jnp.sum(s, axis=0, keepdims=True) for s in sums]
    lane = lax.broadcasted_iota(jnp.int32, (1, 128), 1) // 32
    packed = jnp.zeros((1, 128), jnp.float32)
    for k, row in enumerate(rows):
        row = row + pltpu.roll(row, 64, 1)
        row = row + pltpu.roll(row, 32, 1)
        packed = jnp.where(lane == k, row, packed)
    tile[...] = packed

    def tell(offset, carry):
        peer = lax.rem(me + offset, count)
        pltpu.make_async_remote_copy(
            src_ref=tile, dst_ref=tiles.at[offset - 1],
            send_sem=tile_send, recv_sem=tile_recv,
            device_id=(peer // lon, lax.rem(peer, lon)), device_id_type=MESH,
        ).start()
        return carry

    lax.fori_loop(1, count, tell, 0)
    for group in (sum0, sum1, direct, relayed0, relayed1, own_a, own_b):
        for copy in group.values():
            copy.wait_send()
    everything = pltpu.make_async_remote_copy(
        src_ref=tiles, dst_ref=tiles, send_sem=tile_send, recv_sem=tile_recv,
        device_id=right_dev, device_id_type=MESH,
    )
    everything.wait_send()
    everything.wait_recv()
    total = jnp.sum(tiles[...], axis=0) + tile[...]
    norm_old, curvature, cross_term, square = (
        jnp.sum(jnp.where(lane == k, total, 0.0), axis=1, keepdims=True) for k in range(4)
    )
    step_size = norm_old / curvature
    norm_new = norm_old - 2.0 * step_size * cross_term + step_size * step_size * square
    step_row[...] = jnp.broadcast_to(step_size, step_row.shape)
    ratio_row[...] = jnp.broadcast_to(norm_new / norm_old, ratio_row.shape)


def body(ens, lon, control, residual, direction, ens_perturb, localize, obs_cell, obs_slot, obs_weight):
    flip = functools.partial(jnp.swapaxes, axis1=-1, axis2=-2)
    control, residual, direction, ens_perturb = map(flip, (control, residual, direction, ens_perturb))
    members, cols, lat = direction.shape
    nobs = obs_cell.shape[0]
    block = lat // ens
    na, nb = factors(ens)
    pa, pb = max(na - 1, 1), max(nb - 1, 1)
    count = ens * lon
    wide = cols + 2 * HALO
    f32, bf16 = jnp.float32, jnp.bfloat16
    vmem = pl.BlockSpec(memory_space=pltpu.VMEM)
    outside = pl.BlockSpec(memory_space=pl.ANY)
    dma = pltpu.SemaphoreType.DMA
    row = jax.ShapeDtypeStruct((1, lat), f32)
    image, step_size, ratio = pl.pallas_call(
        functools.partial(kernel, ens, lon),
        out_shape=(jax.ShapeDtypeStruct((members, cols, lat), f32), row, row),
        in_specs=[vmem, outside, outside, outside] + [vmem] * 4,
        out_specs=(vmem, vmem, vmem),
        scratch_shapes=[
            pltpu.VMEM((lat, lat), f32),
            pltpu.VMEM((members, cols, lat), f32),
            pltpu.VMEM((members, 3, cols, lat), bf16),
            pltpu.VMEM((lat, lat), bf16),
            pltpu.VMEM((lat, lat), bf16),
            pltpu.VMEM((2 * members * cols, lat), bf16),
            pltpu.VMEM((ens, 3, cols, block), f32),
            pltpu.VMEM((pb, pa, 3, cols // 2, block), f32),
            pltpu.VMEM((pa, pb, 3, cols // 2, block), f32),
            pltpu.VMEM((pa, 3, cols, block), f32),
            pltpu.VMEM((pb, 3, cols, block), f32),
            pltpu.VMEM((3, cols, block), f32),
            pltpu.VMEM((3, wide, lat), f32),
            pltpu.VMEM((3, wide, lat), f32),
            pltpu.VMEM((STEPS, wide, lat), f32),
            pltpu.VMEM((2 * STEPS * cols, lat), f32),
            pltpu.VMEM((STEPS, wide, lat), f32),
            pltpu.VMEM((count - 1, 1, 128), f32),
            pltpu.VMEM((1, 128), f32),
            dma((ens + 2,)), dma((copy_count(ens),)), dma((copy_count(ens),)),
            dma, dma,
        ],
        compiler_params=pltpu.CompilerParams(collective_id=0, has_side_effects=True),
    )(
        direction, residual, ens_perturb, localize,
        obs_cell.reshape(1, nobs), obs_slot.reshape(1, nobs), obs_weight.reshape(1, nobs),
        jnp.asarray(grid_constants(lat)),
    )
    control_new = control + step_size * direction
    residual_new = residual - step_size * image
    direction_new = residual_new + ratio * direction
    return tuple(map(flip, (control_new, residual_new, direction_new)))


def solution(mesh):
    fields = P("ens", None, "lon")
    in_specs = (fields, fields, fields, P("ens", None, None, "lon"), P(), P("lon"), P("lon"), P("lon"))
    ens, lon = mesh.shape["ens"], mesh.shape["lon"]
    return jax.shard_map(
        functools.partial(body, ens, lon), mesh=mesh, in_specs=in_specs,
        out_specs=(fields, fields, fields), check_vma=False,
    )
```

```python
import functools
import itertools

import numpy as np
import jax
import jax.numpy as jnp
from jax import lax
from jax.experimental import pallas as pl
from jax.experimental.pallas import tpu as pltpu
from jax.sharding import PartitionSpec as P

STEPS = 3
HALO = 8
CHUNK = 512
MESH = pl.DeviceIdType.MESH
NT = (((1,), (1,)), ((), ()))
NN = (((1,), (0,)), ((), ()))


def split_bf16(values):
    high = values.astype(jnp.bfloat16)
    low = (values - high.astype(jnp.float32)).astype(jnp.bfloat16)
    return high, low


def dot(left, right, dims):
    return lax.dot_general(left, right, dims, preferred_element_type=jnp.float32)


def grid_constants(lat):
    phi = np.pi * (-1.0 / 3.0 + 2.0 / 3.0 * (np.arange(lat) + 0.5) / lat)
    half = 0.5 * 0.35
    up = np.full(lat, half)
    up[-1] = 0.0
    down = np.full(lat, half)
    down[0] = 0.0
    rows = np.stack([half / np.cos(phi), 0.2 * np.sin(phi), up, down])
    return np.ascontiguousarray(np.broadcast_to(rows[:, None], (4, 8, lat))).astype(np.float32)


def linear_step(source, target, sign, consts, blocks):
    rows, lat = source.shape[1], source.shape[2]
    lon_c, cor_c, up_c, down_c = (sign * consts[k] for k in range(4))
    for start in blocks:
        here = pl.ds(start, 8)

        def east(comp, block):
            if start + 8 == rows:
                return pltpu.roll(block, 7, 0)
            return source[comp, pl.ds(start + 1, 8), :]

        def west(comp, block):
            if start == 0:
                return pltpu.roll(block, 1, 0)
            return source[comp, pl.ds(start - 1, 8), :]

        def lat_diff(block):
            return up_c * pltpu.roll(block, lat - 1, 1) - down_c * pltpu.roll(block, 1, 1)

        height, zonal, merid = (source[c, here, :] for c in range(3))
        height_lon = east(0, height) - west(0, height)
        zonal_lon = east(1, zonal) - west(1, zonal)
        target[0, here, :] = height - lon_c * zonal_lon - lat_diff(merid)
        target[1, here, :] = zonal - lon_c * height_lon + cor_c * merid
        target[2, here, :] = merid - lat_diff(height) - cor_c * zonal


def factors(ens):
    first = 2 if ens % 2 == 0 else 1
    return first, ens // first


def copy_count(ens):
    na, nb = factors(ens)
    cross = (na - 1) * (nb - 1)
    return 3 * (4 * cross + 3 * (na - 1 + nb - 1)) + 8


def kernel(
    ens, lon, direction, residual_hbm, perturb_hbm, localize_hbm, cell, slot, weight, consts,
    image, step_row, ratio_row,
    localize, residual, perturb, high, low, split, stage, relay0, relay1, arr_a, arr_b,
    reduced, fields, other, heights, wsum, wmat, tiles, tile,
    load_sem, send_sem, recv_sem, tile_send, tile_recv,
):
    na, nb = factors(ens)
    me_e, me_l = lax.axis_index("ens"), lax.axis_index("lon")
    me_a, me_b = me_e // nb, lax.rem(me_e, nb)
    count = ens * lon
    me = me_e * lon + me_l
    members, cols, lat = direction.shape
    block = lat // ens
    half = cols // 2
    stacked = members * cols
    halves = (pl.ds(0, half), pl.ds(half, half))
    inner = (pl.ds(HALO, half), pl.ds(HALO + half, half))

    def ens_of(i, j):
        return lax.rem(me_a + i, na) * nb + lax.rem(me_b + j, nb)

    def lanes_of(index):
        return pl.ds(pl.multiple_of(index * block, block), block)

    order = [(i, j) for i in range(1, na) for j in range(1, nb)]
    order += [(0, j) for j in range(1, nb)] + [(i, 0) for i in range(1, na)] + [(0, 0)]

    loads = {}
    for k, (i, j) in enumerate(order):
        at = lanes_of(ens_of(i, j))
        loads[i, j] = pltpu.make_async_copy(localize_hbm.at[at, :], localize.at[at, :], load_sem.at[k])
    load_p = pltpu.make_async_copy(perturb_hbm, perturb, load_sem.at[ens])
    load_r = pltpu.make_async_copy(residual_hbm, residual, load_sem.at[ens + 1])
    loads[order[0]].start()
    load_p.start()
    for key in order[1:]:
        loads[key].start()
    load_r.start()

    barrier = pltpu.get_barrier_semaphore()

    def greet(offset, carry):
        peer = lax.rem(me + offset, count)
        pl.semaphore_signal(
            barrier, inc=1, device_id=(peer // lon, lax.rem(peer, lon)), device_id_type=MESH
        )
        return carry

    lax.fori_loop(1, count, greet, 0)

    ids = itertools.count()

    def remote(src, dst, device):
        k = next(ids)
        return pltpu.make_async_remote_copy(
            src_ref=src, dst_ref=dst, send_sem=send_sem.at[k], recv_sem=recv_sem.at[k],
            device_id=device, device_id_type=MESH,
        )

    d_high, d_low = split_bf16(direction[...].reshape(stacked, lat))
    split[pl.ds(0, stacked), :] = d_high
    split[pl.ds(stacked, stacked), :] = d_low

    def localized_block(i, j):
        index = ens_of(i, j)
        at = lanes_of(index)
        loads[i, j].wait()
        l_high, l_low = split_bf16(localize[at, :])
        high[at, :] = l_high
        low[at, :] = l_low
        both = dot(split[...], l_high, NT)
        local = both[:stacked] + both[stacked:] + dot(split[pl.ds(0, stacked), :], l_low, NT)
        if (i, j) == order[0]:
            load_p.wait()
        for c in range(3):
            total = None
            for m in range(members):
                term = perturb[m, c, :, at].astype(jnp.float32) * local[m * cols:(m + 1) * cols]
                total = term if total is None else total + term
            stage[i * nb + j, c] = total

    def a_peer(i):
        return (ens_of(i, 0), me_l)

    def b_peer(j):
        return (ens_of(0, j), me_l)

    def part(i, j, c, h):
        return stage.at[i * nb + j, c, halves[h]]

    sum0, sum1, direct, relayed0, relayed1 = {}, {}, {}, {}, {}
    for c in range(3):
        for i in range(1, na):
            for j in range(1, nb):
                sum0[i, j, c] = remote(part(i, j, c, 0), relay0.at[j - 1, i - 1, c], b_peer(j))
                sum1[i, j, c] = remote(part(i, j, c, 1), relay1.at[i - 1, j - 1, c], a_peer(i))
        for j in range(1, nb):
            direct[0, j, c] = remote(part(0, j, c, 0), arr_b.at[j - 1, c, halves[0]], b_peer(j))
            relayed1[j, c] = remote(part(0, j, c, 1), arr_b.at[j - 1, c, halves[1]], b_peer(j))
        for i in range(1, na):
            direct[i, 0, c] = remote(part(i, 0, c, 1), arr_a.at[i - 1, c, halves[1]], a_peer(i))
            relayed0[i, c] = remote(part(i, 0, c, 0), arr_a.at[i - 1, c, halves[0]], a_peer(i))

    for k, (i, j) in enumerate(order):
        localized_block(i, j)
        if k == 0:
            pl.semaphore_wait(barrier, count - 1)
        for c in range(3):
            if i and j:
                sum0[i, j, c].start()
                sum1[i, j, c].start()
            elif i or j:
                direct[i, j, c].start()

    wsum[...] = jnp.zeros_like(wsum)
    slots_cols = STEPS * cols

    def weights(step, carry):
        at = pl.ds(pl.multiple_of(step * CHUNK, CHUNK), CHUNK)
        cells, slots, value = cell[:, at], slot[:, at], weight[:, at]
        row = cells // cols
        key = slots * cols + (cells - row * cols)
        v_high, v_low = split_bf16(value)
        v_high, v_low = v_high.astype(jnp.float32), v_low.astype(jnp.float32)
        ids = lax.broadcasted_iota(jnp.int32, (slots_cols, CHUNK), 0)
        hit = ids == key
        left = jnp.concatenate(
            [jnp.where(hit, v_high, 0.0), jnp.where(hit, v_low, 0.0)], axis=0
        ).astype(jnp.bfloat16)
        lat_ids = lax.broadcasted_iota(jnp.int32, (lat, CHUNK), 0)
        right = jnp.where(lat_ids == row, 1.0, 0.0).astype(jnp.bfloat16)
        wsum[...] += dot(left, right, NT)
        return carry

    chunks = cell.shape[1] // CHUNK
    early, late = chunks * 3 // 8, chunks * 5 // 8
    lax.fori_loop(0, early, weights, 0)

    for c in range(3):
        for i in range(1, na):
            for j in range(1, nb):
                sum0[i, j, c].wait_recv()
                stage[i * nb, c, halves[0]] += relay0[j - 1, i - 1, c]
            relayed0[i, c].start()
        for j in range(1, nb):
            for i in range(1, na):
                sum1[i, j, c].wait_recv()
                stage[j, c, halves[1]] += relay1[i - 1, j - 1, c]
            relayed1[j, c].start()

    lax.fori_loop(early, late, weights, 0)

    left_dev = (me_e, lax.rem(me_l + lon - 1, lon))
    right_dev = (me_e, lax.rem(me_l + 1, lon))

    def halo_copies(ref, which):
        return (
            remote(ref.at[which, pl.ds(HALO, HALO), :], ref.at[which, pl.ds(HALO + cols, HALO), :], left_dev),
            remote(ref.at[which, pl.ds(cols, HALO), :], ref.at[which, pl.ds(0, HALO), :], right_dev),
        )

    mine = lanes_of(me_e)
    own_a, own_b, pass_a, pass_b = {}, {}, {}, {}
    for c in range(3):
        whole = fields.at[c, pl.ds(HALO, cols), mine]
        for i in range(1, na):
            own_a[i, c] = remote(reduced.at[c], whole, a_peer(i))
        for j in range(1, nb):
            own_b[j, c] = remote(reduced.at[c], whole, b_peer(j))
        for i in range(1, na):
            for j in range(1, nb):
                from_b = lanes_of(me_a * nb + lax.rem(me_b + nb - j, nb))
                from_a = lanes_of(lax.rem(me_a + na - i, na) * nb + me_b)
                spot0 = fields.at[c, inner[0], from_b]
                spot1 = fields.at[c, inner[1], from_a]
                pass_a[i, j, c] = remote(spot0, spot0, a_peer(i))
                pass_b[i, j, c] = remote(spot1, spot1, b_peer(j))

    for c in range(3):
        total = stage[0, c]
        for j in range(1, nb):
            direct[0, j, c].wait_recv()
            relayed1[j, c].wait_recv()
            total = total + arr_b[j - 1, c]
        for i in range(1, na):
            direct[i, 0, c].wait_recv()
            relayed0[i, c].wait_recv()
            total = total + arr_a[i - 1, c]
        reduced[c] = total
        fields[c, pl.ds(HALO, cols), mine] = total
        for copy in [own_a[i, c] for i in range(1, na)] + [own_b[j, c] for j in range(1, nb)]:
            copy.start()
    lax.fori_loop(late, chunks, weights, 0)
    for s in range(STEPS):
        wmat[s, pl.ds(HALO, cols), :] = (
            wsum[pl.ds(s * cols, cols), :] + wsum[pl.ds(slots_cols + s * cols, cols), :]
        )

    w_copies = (
        remote(wmat.at[:, pl.ds(HALO, HALO), :], wmat.at[:, pl.ds(HALO + cols, HALO), :], left_dev),
        remote(wmat.at[:, pl.ds(cols, HALO), :], wmat.at[:, pl.ds(0, HALO), :], right_dev),
    )
    for copy in w_copies:
        copy.start()

    load_r.wait()
    for c in range(3):
        for j in range(1, nb):
            own_b[j, c].wait_recv()
            for i in range(1, na):
                pass_a[i, j, c].start()
        for i in range(1, na):
            own_a[i, c].wait_recv()
            for j in range(1, nb):
                pass_b[i, j, c].start()
    f_copies = []
    for c in range(3):
        for i in range(1, na):
            for j in range(1, nb):
                pass_a[i, j, c].wait_recv()
                pass_b[i, j, c].wait_recv()
        for copy in halo_copies(fields, c):
            copy.start()
            f_copies.append(copy)
    for group in (pass_a, pass_b):
        for copy in group.values():
            copy.wait_send()
    wide = fields.shape[1]
    every = range(0, wide, 8)

    def forward(source, target, n, blocks):
        linear_step(source, target, 1.0, consts, blocks)
        for start in blocks:
            heights[n, pl.ds(start, 8), :] = target[0, pl.ds(start, 8), :]

    inside = [range(HALO + 8 * (n + 1), wide - HALO - 8 * (n + 1), 8) for n in range(STEPS)]
    outer = [[start for start in every if start not in inside[n]] for n in range(STEPS)]
    buffers = (fields, other, fields, other)
    for n in range(STEPS):
        forward(buffers[n], buffers[n + 1], n, inside[n])
    for copy in f_copies:
        copy.wait()
    for n in range(STEPS):
        forward(buffers[n], buffers[n + 1], n, outer[n])
    for copy in w_copies:
        copy.wait()
    fields[0] = wmat[2] * heights[2]
    fields[1] = jnp.zeros_like(fields[1])
    fields[2] = jnp.zeros_like(fields[2])
    linear_step(fields, other, -1.0, consts, every)
    other[0] += wmat[1] * heights[1]
    linear_step(other, fields, -1.0, consts, every)
    fields[0] += wmat[0] * heights[0]
    linear_step(fields, other, -1.0, consts, every)

    for m in range(members):
        total = None
        for c in range(3):
            term = perturb[m, c].astype(jnp.float32) * other[c, pl.ds(HALO, cols), :]
            total = term if total is None else total + term
        p_high, p_low = split_bf16(total)
        split[pl.ds(m * cols, cols), :] = p_high
        split[pl.ds(stacked + m * cols, cols), :] = p_low

    def pulled(index, sums):
        at = lanes_of(index)
        both = dot(split[...], high[:, at], NN)
        back = both[:stacked] + both[stacked:] + dot(split[pl.ds(0, stacked), :], low[:, at], NN)
        out = []
        d = direction[:, :, at].reshape(stacked, block)
        r = residual[:, :, at].reshape(stacked, block)
        img = d + back
        image[:, :, at] = img.reshape(members, cols, block)
        for total, term in zip(sums, (r * r, d * img, r * img, img * img)):
            term = term.reshape(stacked // 8, 8, block).sum(axis=0)
            for k in range(block // 128):
                total = total + term[:, k * 128:(k + 1) * 128]
            out.append(total)
        return tuple(out)

    sums = lax.fori_loop(0, ens, pulled, tuple(jnp.zeros((8, 128), jnp.float32) for _ in range(4)))
    rows = [jnp.sum(s, axis=0, keepdims=True) for s in sums]
    lane = lax.broadcasted_iota(jnp.int32, (1, 128), 1) // 32
    packed = jnp.zeros((1, 128), jnp.float32)
    for k, row in enumerate(rows):
        row = row + pltpu.roll(row, 64, 1)
        row = row + pltpu.roll(row, 32, 1)
        packed = jnp.where(lane == k, row, packed)
    tile[...] = packed

    def tell(offset, carry):
        peer = lax.rem(me + offset, count)
        pltpu.make_async_remote_copy(
            src_ref=tile, dst_ref=tiles.at[offset - 1],
            send_sem=tile_send, recv_sem=tile_recv,
            device_id=(peer // lon, lax.rem(peer, lon)), device_id_type=MESH,
        ).start()
        return carry

    lax.fori_loop(1, count, tell, 0)
    for group in (sum0, sum1, direct, relayed0, relayed1, own_a, own_b):
        for copy in group.values():
            copy.wait_send()
    everything = pltpu.make_async_remote_copy(
        src_ref=tiles, dst_ref=tiles, send_sem=tile_send, recv_sem=tile_recv,
        device_id=right_dev, device_id_type=MESH,
    )
    everything.wait_send()
    everything.wait_recv()
    total = jnp.sum(tiles[...], axis=0) + tile[...]
    norm_old, curvature, cross_term, square = (
        jnp.sum(jnp.where(lane == k, total, 0.0), axis=1, keepdims=True) for k in range(4)
    )
    step_size = norm_old / curvature
    norm_new = norm_old - 2.0 * step_size * cross_term + step_size * step_size * square
    step_row[...] = jnp.broadcast_to(step_size, step_row.shape)
    ratio_row[...] = jnp.broadcast_to(norm_new / norm_old, ratio_row.shape)


def body(ens, lon, control, residual, direction, ens_perturb, localize, obs_cell, obs_slot, obs_weight):
    flip = functools.partial(jnp.swapaxes, axis1=-1, axis2=-2)
    control, residual, direction, ens_perturb = map(flip, (control, residual, direction, ens_perturb))
    members, cols, lat = direction.shape
    nobs = obs_cell.shape[0]
    block = lat // ens
    na, nb = factors(ens)
    pa, pb = max(na - 1, 1), max(nb - 1, 1)
    count = ens * lon
    wide = cols + 2 * HALO
    f32, bf16 = jnp.float32, jnp.bfloat16
    vmem = pl.BlockSpec(memory_space=pltpu.VMEM)
    outside = pl.BlockSpec(memory_space=pl.ANY)
    dma = pltpu.SemaphoreType.DMA
    row = jax.ShapeDtypeStruct((1, lat), f32)
    image, step_size, ratio = pl.pallas_call(
        functools.partial(kernel, ens, lon),
        out_shape=(jax.ShapeDtypeStruct((members, cols, lat), f32), row, row),
        in_specs=[vmem, outside, outside, outside] + [vmem] * 4,
        out_specs=(vmem, vmem, vmem),
        scratch_shapes=[
            pltpu.VMEM((lat, lat), f32),
            pltpu.VMEM((members, cols, lat), f32),
            pltpu.VMEM((members, 3, cols, lat), bf16),
            pltpu.VMEM((lat, lat), bf16),
            pltpu.VMEM((lat, lat), bf16),
            pltpu.VMEM((2 * members * cols, lat), bf16),
            pltpu.VMEM((ens, 3, cols, block), f32),
            pltpu.VMEM((pb, pa, 3, cols // 2, block), f32),
            pltpu.VMEM((pa, pb, 3, cols // 2, block), f32),
            pltpu.VMEM((pa, 3, cols, block), f32),
            pltpu.VMEM((pb, 3, cols, block), f32),
            pltpu.VMEM((3, cols, block), f32),
            pltpu.VMEM((3, wide, lat), f32),
            pltpu.VMEM((3, wide, lat), f32),
            pltpu.VMEM((STEPS, wide, lat), f32),
            pltpu.VMEM((2 * STEPS * cols, lat), f32),
            pltpu.VMEM((STEPS, wide, lat), f32),
            pltpu.VMEM((count - 1, 1, 128), f32),
            pltpu.VMEM((1, 128), f32),
            dma((ens + 2,)), dma((copy_count(ens),)), dma((copy_count(ens),)),
            dma, dma,
        ],
        compiler_params=pltpu.CompilerParams(collective_id=0, has_side_effects=True),
    )(
        direction, residual, ens_perturb, localize,
        obs_cell.reshape(1, nobs), obs_slot.reshape(1, nobs), obs_weight.reshape(1, nobs),
        jnp.asarray(grid_constants(lat)),
    )
    control_new = control + step_size * direction
    residual_new = residual - step_size * image
    direction_new = residual_new + ratio * direction
    return tuple(map(flip, (control_new, residual_new, direction_new)))


def solution(mesh):
    fields = P("ens", None, "lon")
    in_specs = (fields, fields, fields, P("ens", None, None, "lon"), P(), P("lon"), P("lon"), P("lon"))
    ens, lon = mesh.shape["ens"], mesh.shape["lon"]
    return jax.shard_map(
        functools.partial(body, ens, lon), mesh=mesh, in_specs=in_specs,
        out_specs=(fields, fields, fields), check_vma=False,
    )
```
